32 devices in a mesh: dp: 4 (over z), tp: 8 (over y, x, core).
Axes of the slice: x: 2, y: 2, z: 4, core: 2. Of those that a mesh axis runs over, the one named last changes fastest.
Arguments:
- hidden: bfloat16 [512, 128, 1024], P('dp')
- positions: int32 [512, 20], P('dp')
- labels: int32 [512, 20], P('dp')
- weights: float32 [512, 20], P('dp')
- w_t: bfloat16 [1024, 1024], replicated
- b_t: float32 [1024], replicated
- gamma: float32 [1024], replicated
- beta: float32 [1024], replicated
- embed: bfloat16 [30592, 1024], P('tp')
- out_bias: float32 [30592], P('tp')
Outputs:
- output 1: float32 [], replicated
- output 2: bfloat16 [512, 128, 1024], P('dp')
- output 3: float32 [1024, 1024], replicated
- output 4: float32 [1024], replicated
- output 5: float32 [1024], replicated
- output 6: float32 [1024], replicated
- output 7: float32 [30592, 1024], P('tp')
- output 8: float32 [30592], P('tp')
All inputs are finite; a program needn't handle non-finite values.
Results may differ from the reference program's by a relative error of at most 0.001.
Values sent between devices are 32-bit elements.
A program may use at most 1 GiB of HBM per device.

```python
import jax
import jax.numpy as jnp
from jax import lax

HIDDEN = 1024
VOCAB_REAL = 30522
VOCAB_PAD = 30592
SEQ_LEN = 128
MAX_PRED = 20
BATCH_TOTAL = 512
BLOCK_SEQ = 8
NUM_BLOCKS = BATCH_TOTAL // BLOCK_SEQ
BLOCK_ROWS = BLOCK_SEQ * MAX_PRED
LN_EPS = 1e-12
LOSS_EPS = 1e-5


def setup_inputs(seed: int = 0) -> dict:
    key = jax.random.key(seed)
    keys = jax.random.split(key, 10)
    hidden = jax.random.normal(keys[0], (BATCH_TOTAL, SEQ_LEN, HIDDEN), jnp.float32).astype(jnp.bfloat16)
    row_keys = jax.random.split(keys[1], BATCH_TOTAL)
    positions = jax.vmap(lambda row_key: jax.random.permutation(row_key, SEQ_LEN)[:MAX_PRED])(row_keys).astype(jnp.int32)
    labels = jax.random.randint(keys[2], (BATCH_TOTAL, MAX_PRED), 0, VOCAB_REAL, dtype=jnp.int32)
    pred_counts = jax.random.randint(keys[3], (BATCH_TOTAL,), 1, MAX_PRED + 1, dtype=jnp.int32).at[0].set(MAX_PRED)
    weights = (jnp.arange(MAX_PRED, dtype=jnp.int32)[None, :] < pred_counts[:, None]).astype(jnp.float32)
    w_t = (jax.random.normal(keys[4], (HIDDEN, HIDDEN), jnp.float32) * HIDDEN ** -0.5).astype(jnp.bfloat16)
    b_t = 0.5 * jax.random.normal(keys[5], (HIDDEN,), jnp.float32)
    gamma = 1.0 + 0.3 * jax.random.normal(keys[6], (HIDDEN,), jnp.float32)
    beta = 0.3 * jax.random.normal(keys[7], (HIDDEN,), jnp.float32)
    embed = (jax.random.normal(keys[8], (VOCAB_PAD, HIDDEN), jnp.float32) * (1.5 * HIDDEN ** -0.5)).astype(jnp.bfloat16)
    raw_bias = 0.5 * jax.random.normal(keys[9], (VOCAB_PAD,), jnp.float32)
    out_bias = jnp.where(jnp.arange(VOCAB_PAD) < VOCAB_REAL, raw_bias, -1e9)
    return {"hidden": hidden, "positions": positions, "labels": labels, "weights": weights, "w_t": w_t, "b_t": b_t, "gamma": gamma, "beta": beta, "embed": embed, "out_bias": out_bias}


def gelu_norm(pre_act, gamma, beta):
    activated = jax.nn.gelu(pre_act, approximate=False)
    mean_val = jnp.mean(activated, axis=-1, keepdims=True)
    centered = activated - mean_val
    variance = jnp.mean(centered * centered, axis=-1, keepdims=True)
    return centered * lax.rsqrt(variance + LN_EPS) * gamma + beta


def reference(hidden, positions, labels, weights, w_t, b_t, gamma, beta, embed, out_bias):
    picked = jnp.take_along_axis(hidden, positions[:, :, None], axis=1)
    tok_rows = picked.reshape(BATCH_TOTAL * MAX_PRED, HIDDEN)
    pre_act = jnp.dot(tok_rows, w_t, preferred_element_type=jnp.float32) + b_t
    normed, norm_vjp = jax.vjp(gelu_norm, pre_act, gamma, beta)
    t_bf = normed.astype(jnp.bfloat16)
    flat_w = weights.reshape(-1)
    denom = jnp.sum(flat_w) + LOSS_EPS
    vocab_ids = jnp.arange(VOCAB_PAD, dtype=jnp.int32)

    def block_step(carry, block):
        d_embed, d_bias, loss_sum = carry
        t_blk, lab_blk, w_blk = block
        logits = jnp.dot(t_blk, embed.T, preferred_element_type=jnp.float32) + out_bias
        row_max = jnp.max(logits, axis=1)
        shifted = jnp.exp(logits - row_max[:, None])
        sum_exp = jnp.sum(shifted, axis=1)
        log_norm = jnp.log(sum_exp) + row_max
        lab_hot = lab_blk[:, None] == vocab_ids[None, :]
        target_logit = jnp.sum(jnp.where(lab_hot, logits, 0.0), axis=1)
        soft_probs = shifted * (1.0 / sum_exp)[:, None]
        d_logits = jnp.where(lab_hot, soft_probs - 1.0, soft_probs) * (w_blk / denom)[:, None]
        dz_bf = d_logits.astype(jnp.bfloat16)
        d_embed = d_embed + jnp.dot(dz_bf.T, t_blk, preferred_element_type=jnp.float32)
        d_bias = d_bias + jnp.sum(d_logits, axis=0)
        loss_sum = loss_sum + jnp.sum(w_blk * (log_norm - target_logit))
        d_normed = jnp.dot(dz_bf, embed, preferred_element_type=jnp.float32)
        return (d_embed, d_bias, loss_sum), d_normed

    init = (jnp.zeros((VOCAB_PAD, HIDDEN), jnp.float32), jnp.zeros((VOCAB_PAD,), jnp.float32), jnp.zeros((), jnp.float32))
    blocks = (t_bf.reshape(NUM_BLOCKS, BLOCK_ROWS, HIDDEN), labels.reshape(NUM_BLOCKS, BLOCK_ROWS), flat_w.reshape(NUM_BLOCKS, BLOCK_ROWS))
    (d_embed, d_out_bias, loss_sum), d_normed = lax.scan(block_step, init, blocks)
    loss = loss_sum / denom
    d_pre, d_gamma, d_beta = norm_vjp(d_normed.reshape(BATCH_TOTAL * MAX_PRED, HIDDEN))
    d_pre_bf = d_pre.astype(jnp.bfloat16)
    d_w_t = jnp.dot(tok_rows.T, d_pre_bf, preferred_element_type=jnp.float32)
    d_b_t = jnp.sum(d_pre, axis=0)
    d_rows = jnp.dot(d_pre_bf, w_t.T, preferred_element_type=jnp.float32).astype(jnp.bfloat16)
    row_ids = jnp.arange(BATCH_TOTAL)[:, None]
    d_hidden = jnp.zeros((BATCH_TOTAL, SEQ_LEN, HIDDEN), jnp.bfloat16).at[row_ids, positions].add(d_rows.reshape(BATCH_TOTAL, MAX_PRED, HIDDEN))
    return (loss, d_hidden, d_w_t, d_b_t, d_gamma, d_beta, d_embed, d_out_bias)
```

```python
import functools

import jax
import jax.numpy as jnp
from jax import lax
from jax.experimental import pallas as pl
from jax.experimental.pallas import tpu as pltpu
from jax.sharding import PartitionSpec as P

LN_EPS = 1e-12
LOSS_EPS = 1e-5
VMEM_LIMIT = 60 * 1024 * 1024
ROW_CHUNK = 512
BLOCK_N = 512
GROUP = 8


def gelu_norm(pre_act, gamma, beta):
    activated = jax.nn.gelu(pre_act, approximate=False)
    mean_val = jnp.mean(activated, axis=-1, keepdims=True)
    centered = activated - mean_val
    variance = jnp.mean(centered * centered, axis=-1, keepdims=True)
    return centered * lax.rsqrt(variance + LN_EPS) * gamma + beta


def row_chunks(rows):
    return [(start, min(ROW_CHUNK, rows - start)) for start in range(0, rows, ROW_CHUNK)]


def params(**kw):
    return pltpu.CompilerParams(vmem_limit_bytes=VMEM_LIMIT, **kw)


def pick_kernel(rowpos_ref, hid_ref, out_ref):
    rows, depth = out_ref.shape[0], hid_ref.shape[0]
    hot = (rowpos_ref[...] == lax.broadcasted_iota(jnp.int32, (rows, depth), 1)).astype(jnp.bfloat16)
    out_ref[...] = jnp.dot(hot, hid_ref[...], preferred_element_type=jnp.float32).astype(jnp.bfloat16)


def pick(hidden, rowpos):
    groups = hidden.shape[0] // GROUP
    depth = GROUP * hidden.shape[1]
    width = hidden.shape[2]
    rows = rowpos.shape[0] // groups
    return pl.pallas_call(
        pick_kernel,
        grid=(groups,),
        in_specs=[pl.BlockSpec((rows, 1), lambda g: (g, 0)), pl.BlockSpec((depth, width), lambda g: (g, 0))],
        out_specs=pl.BlockSpec((rows, width), lambda g: (g, 0)),
        out_shape=jax.ShapeDtypeStruct((rows * groups, width), jnp.bfloat16),
        compiler_params=params(),
        cost_estimate=pl.CostEstimate(flops=2 * rows * groups * depth * width, bytes_accessed=hidden.size * 2, transcendentals=0),
        name="pick",
    )(rowpos.reshape(-1, 1), hidden.reshape(groups * depth, width))


def put_kernel(rowpos_ref, dh_ref, out_ref):
    depth, rows = out_ref.shape[0], dh_ref.shape[0]
    hot = (rowpos_ref[0] == lax.broadcasted_iota(jnp.int32, (depth, rows), 0)).astype(jnp.bfloat16)
    out_ref[...] = jnp.dot(hot, dh_ref[...].astype(jnp.bfloat16), preferred_element_type=jnp.float32).astype(jnp.bfloat16)


def put(d_rows, rowpos, batch, seq_len):
    groups = batch // GROUP
    depth = GROUP * seq_len
    width = d_rows.shape[1]
    rows = rowpos.shape[0] // groups
    out = pl.pallas_call(
        put_kernel,
        grid=(groups,),
        in_specs=[pl.BlockSpec((1, 1, rows), lambda g: (g, 0, 0)), pl.BlockSpec((rows, width), lambda g: (g, 0))],
        out_specs=pl.BlockSpec((depth, width), lambda g: (g, 0)),
        out_shape=jax.ShapeDtypeStruct((groups * depth, width), jnp.bfloat16),
        compiler_params=params(),
        cost_estimate=pl.CostEstimate(flops=2 * rows * groups * depth * width, bytes_accessed=groups * depth * width * 2, transcendentals=0),
        name="put",
    )(rowpos.reshape(groups, 1, rows), d_rows)
    return out.reshape(batch, seq_len, width)


def logits_kernel(which_ref, t_ref, embed_ref, bias_ref, lab_ref, z_ref, stat_ref):
    del which_ref
    t_blk = t_ref[...].astype(jnp.bfloat16)
    lab = lab_ref[...]
    cols = t_blk.shape[0]
    top = jnp.full((1, cols), -jnp.inf, jnp.float32)
    total = jnp.zeros((1, cols), jnp.float32)
    target = jnp.zeros((1, cols), jnp.float32)
    for start, rows in row_chunks(embed_ref.shape[0]):
        z = lax.dot_general(embed_ref[start:start + rows, :], t_blk, (((1,), (1,)), ((), ())), preferred_element_type=jnp.float32)
        z = z + bias_ref[start:start + rows, :]
        z_ref[start:start + rows, :] = z
        new_top = jnp.maximum(top, jnp.max(z, axis=0, keepdims=True))
        total = total * jnp.exp(top - new_top) + jnp.sum(jnp.exp(z - new_top), axis=0, keepdims=True)
        top = new_top
        hot = lab == lax.broadcasted_iota(jnp.int32, (rows, cols), 0) + start
        target = target + jnp.sum(jnp.where(hot, z, 0.0), axis=0, keepdims=True)
    stat_ref[0:1, :] = top
    stat_ref[1:2, :] = total
    stat_ref[2:3, :] = target
    stat_ref[3:8, :] = jnp.zeros((5, cols), jnp.float32)


def block_map(planes, per_plane):
    if planes == 0:
        return lambda k, which: k
    return lambda k, which: lax.rem(which[0] + 1 + k // per_plane, planes) * per_plane + lax.rem(k, per_plane)


def logits_call(which, t_rows, embed, bias_col, lab_row, planes, per_plane):
    slots = lab_row.shape[1]
    vocab, width = embed.shape
    where = block_map(planes, per_plane)
    return pl.pallas_call(
        logits_kernel,
        grid_spec=pltpu.PrefetchScalarGridSpec(
            num_scalar_prefetch=1,
            grid=(slots // BLOCK_N,),
            in_specs=[
                pl.BlockSpec((BLOCK_N, width), lambda k, which: (where(k, which), 0)),
                pl.BlockSpec((vocab, width), lambda k, which: (0, 0), pipeline_mode=pl.Buffered(1)),
                pl.BlockSpec((vocab, 1), lambda k, which: (0, 0), pipeline_mode=pl.Buffered(1)),
                pl.BlockSpec((1, BLOCK_N), lambda k, which: (0, k)),
            ],
            out_specs=[
                pl.BlockSpec((vocab, BLOCK_N), lambda k, which: (0, k)),
                pl.BlockSpec((8, BLOCK_N), lambda k, which: (0, k)),
            ],
        ),
        out_shape=[jax.ShapeDtypeStruct((vocab, slots), jnp.float32), jax.ShapeDtypeStruct((8, slots), jnp.float32)],
        compiler_params=params(),
        cost_estimate=pl.CostEstimate(flops=2 * slots * vocab * width, bytes_accessed=slots * vocab * 4, transcendentals=slots * vocab),
        name="logits",
    )(which, t_rows, embed, bias_col, lab_row)


def dz_of(z, stat_ref, lab, start):
    soft = jnp.exp(z - stat_ref[0:1, :]) * stat_ref[1:2, :]
    hot = lab == lax.broadcasted_iota(jnp.int32, z.shape, 0) + start
    return jnp.where(hot, soft - 1.0, soft) * stat_ref[2:3, :]


def dt_kernel(z_ref, stat_ref, lab_ref, embed_ref, dt_ref):
    lab = lab_ref[...]
    acc = None
    for start, rows in row_chunks(embed_ref.shape[0]):
        dz = dz_of(z_ref[start:start + rows, :], stat_ref, lab, start).astype(jnp.bfloat16)
        part = lax.dot_general(dz, embed_ref[start:start + rows, :], (((0,), (0,)), ((), ())), preferred_element_type=jnp.float32)
        acc = part if acc is None else acc + part
    dt_ref[...] = acc


def dt_call(z, stat, lab_row, embed):
    slots = z.shape[1]
    vocab, width = embed.shape
    block = 256
    return pl.pallas_call(
        dt_kernel,
        grid=(slots // block,),
        in_specs=[
            pl.BlockSpec((vocab, block), lambda k: (0, k)),
            pl.BlockSpec((8, block), lambda k: (0, k)),
            pl.BlockSpec((1, block), lambda k: (0, k)),
            pl.BlockSpec((vocab, width), lambda k: (0, 0), pipeline_mode=pl.Buffered(1)),
        ],
        out_specs=pl.BlockSpec((block, width), lambda k: (k, 0)),
        out_shape=jax.ShapeDtypeStruct((slots, width), jnp.float32),
        compiler_params=params(),
        cost_estimate=pl.CostEstimate(flops=2 * slots * vocab * width, bytes_accessed=slots * vocab * 4, transcendentals=slots * vocab),
        name="dt",
    )(z, stat, lab_row, embed)


def de_kernel(first, which_ref, z_ref, stat_ref, lab_ref, t_ref, *rest):
    del which_ref
    if first:
        de_ref, db_ref = rest
    else:
        de_in, db_in, de_ref, db_ref, sems = rest
    k = pl.program_id(0)

    @pl.when(k == 0)
    def _():
        if first:
            de_ref[...] = jnp.zeros_like(de_ref)
            db_ref[...] = jnp.zeros_like(db_ref)
        else:
            one = pltpu.make_async_copy(de_in, de_ref, sems.at[0])
            two = pltpu.make_async_copy(db_in, db_ref, sems.at[1])
            one.start()
            two.start()
            one.wait()
            two.wait()

    lab = lab_ref[...]
    t_blk = t_ref[...].astype(jnp.bfloat16)
    for start, rows in row_chunks(z_ref.shape[0]):
        dz = dz_of(z_ref[start:start + rows, :], stat_ref, lab, start)
        lanes = dz[:, 0:128]
        for c in range(128, dz.shape[1], 128):
            lanes = lanes + dz[:, c:c + 128]
        db_ref[start:start + rows, :] += lanes
        de_ref[start:start + rows, :] += jnp.dot(dz.astype(jnp.bfloat16), t_blk, preferred_element_type=jnp.float32)


def de_call(which, z, stat, lab_row, t_rows, planes, per_plane, carry=None):
    vocab, slots = z.shape
    width = t_rows.shape[1]
    where = block_map(planes, per_plane)
    first = carry is None
    in_specs = [
        pl.BlockSpec((vocab, BLOCK_N), lambda k, which: (0, k)),
        pl.BlockSpec((8, BLOCK_N), lambda k, which: (0, k)),
        pl.BlockSpec((1, BLOCK_N), lambda k, which: (0, k)),
        pl.BlockSpec((BLOCK_N, width), lambda k, which: (where(k, which), 0)),
    ]
    args = [which, z, stat, lab_row, t_rows]
    scratch = []
    if not first:
        in_specs += [pl.BlockSpec(memory_space=pl.ANY), pl.BlockSpec(memory_space=pl.ANY)]
        args += list(carry)
        scratch = [pltpu.SemaphoreType.DMA((2,))]
    return pl.pallas_call(
        functools.partial(de_kernel, first),
        grid_spec=pltpu.PrefetchScalarGridSpec(
            num_scalar_prefetch=1,
            grid=(slots // BLOCK_N,),
            in_specs=in_specs,
            out_specs=[
                pl.BlockSpec((vocab, width), lambda k, which: (0, 0), pipeline_mode=pl.Buffered(1)),
                pl.BlockSpec((vocab, 128), lambda k, which: (0, 0), pipeline_mode=pl.Buffered(1)),
            ],
            scratch_shapes=scratch,
        ),
        out_shape=[jax.ShapeDtypeStruct((vocab, width), jnp.float32), jax.ShapeDtypeStruct((vocab, 128), jnp.float32)],
        compiler_params=params(),
        cost_estimate=pl.CostEstimate(flops=2 * slots * vocab * width, bytes_accessed=slots * vocab * 4, transcendentals=slots * vocab),
        name="de",
    )(*args)


def combine(stat, weights_row, denom):
    parts = lax.all_gather(stat[:3], "tp", axis=0)
    top = jnp.max(parts[:, 0], axis=0)
    total = jnp.sum(parts[:, 1] * jnp.exp(parts[:, 0] - top[None]), axis=0)
    target = jnp.sum(parts[:, 2], axis=0)
    zero = jnp.zeros_like(top)
    rows = jnp.stack([top, 1.0 / total, weights_row / denom, zero, zero, zero, zero, zero])
    return rows, jnp.log(total) + top - target


def solution(mesh):
    dp, tp = mesh.shape["dp"], mesh.shape["tp"]

    def local_step(hidden, positions, labels, weights, w_t, b_t, gamma, beta, embed, out_bias):
        batch, seq_len, width = hidden.shape
        max_pred = positions.shape[1]
        shard_vocab = embed.shape[0]
        slots = batch * max_pred
        share = slots // tp
        per_plane = slots // BLOCK_N
        dp_idx, tp_idx = lax.axis_index("dp"), lax.axis_index("tp")
        which = dp_idx.reshape(1).astype(jnp.int32)

        small = jnp.stack([labels.reshape(-1).astype(jnp.float32), weights.reshape(-1)])
        small = lax.all_gather(small, "dp", axis=0)
        denom = jnp.sum(small[:, 1]) + LOSS_EPS
        ring = lax.dynamic_slice_in_dim(jnp.concatenate([small, small]), dp_idx + 1, dp - 1, 0)
        far_lab = (ring[:, 0].reshape(1, -1)).astype(jnp.int32) - tp_idx * shard_vocab
        far_w = ring[:, 1].reshape(-1)
        own_lab = labels.reshape(1, -1) - tp_idx * shard_vocab
        own_w = weights.reshape(-1)

        rowpos = (positions + (jnp.arange(batch, dtype=jnp.int32) % GROUP * seq_len)[:, None]).reshape(-1)
        bias_col = out_bias.reshape(-1, 1)

        tok_rows = pick(hidden, rowpos)
        normed = gelu_norm(jnp.dot(tok_rows, w_t, preferred_element_type=jnp.float32) + b_t, gamma, beta)
        t_own = normed.astype(jnp.bfloat16)
        t_part = lax.dynamic_slice_in_dim(t_own, tp_idx * share, share, 0)
        t_part = lax.optimization_barrier(t_part.astype(jnp.float32))
        t_all = lax.all_gather(t_part, ("dp", "tp"), axis=0, tiled=True)

        z_own, stat_own = logits_call(which, t_own, embed, bias_col, own_lab, 0, per_plane)
        rows_own, ce = combine(stat_own, own_w, denom)
        dt_part = dt_call(z_own, rows_own, own_lab, embed)
        carry = de_call(which, z_own, rows_own, own_lab, t_own, 0, per_plane)
        loss = jnp.sum(own_w * ce)

        t_all, carry, dt_part = lax.optimization_barrier((t_all, carry, dt_part))
        d_normed = lax.psum_scatter(dt_part, "tp", scatter_dimension=0, tiled=True)
        z_far, stat_far = logits_call(which, t_all, embed, bias_col, far_lab, dp, per_plane)
        rows_far, _ = combine(stat_far, far_w, denom)
        d_embed, d_bias = de_call(which, z_far, rows_far, far_lab, t_all, dp, per_plane, carry)
        d_out_bias = jnp.sum(d_bias, axis=1)

        part_rows = lax.dynamic_slice_in_dim(tok_rows, tp_idx * share, share, 0)
        pre_act = jnp.dot(part_rows, w_t, preferred_element_type=jnp.float32) + b_t
        _, norm_vjp = jax.vjp(gelu_norm, pre_act, gamma, beta)
        d_pre, d_gamma, d_beta = norm_vjp(d_normed)
        d_pre_bf = d_pre.astype(jnp.bfloat16)
        d_rows = jnp.einsum("ne,de->nd", d_pre_bf, w_t, preferred_element_type=jnp.float32).astype(jnp.bfloat16)
        d_rows = lax.optimization_barrier(d_rows.astype(jnp.float32))
        d_rows = lax.all_gather(d_rows, "tp", axis=0, tiled=True)
        d_w_t = jnp.einsum("nd,ne->de", part_rows, d_pre_bf, preferred_element_type=jnp.float32)
        d_b_t = jnp.sum(d_pre, axis=0)
        loss = jnp.where(tp_idx == 0, loss, 0.0)
        vecs = jnp.stack([d_b_t, d_gamma, d_beta, jnp.full_like(d_b_t, loss)])
        d_w_t, vecs = lax.psum((d_w_t, vecs), ("dp", "tp"))
        d_hidden = put(d_rows, rowpos, batch, seq_len)
        return vecs[3, 0] / denom, d_hidden, d_w_t, vecs[0], vecs[1], vecs[2], d_embed, d_out_bias

    in_specs = (P("dp", None, None), P("dp", None), P("dp", None), P("dp", None), P(None, None), P(None), P(None), P(None), P("tp", None), P("tp"))
    out_specs = (P(), P("dp", None, None), P(None, None), P(None), P(None), P(None), P("tp", None), P("tp"))
    return jax.shard_map(local_step, mesh=mesh, in_specs=in_specs, out_specs=out_specs, check_vma=False)
```

```python
import functools

import jax
import jax.numpy as jnp
from jax import lax
from jax.experimental import pallas as pl
from jax.experimental.pallas import tpu as pltpu
from jax.sharding import PartitionSpec as P

LN_EPS = 1e-12
LOSS_EPS = 1e-5
VMEM_LIMIT = 60 * 1024 * 1024
ROW_CHUNK = 512
BLOCK_N = 512
DT_BLOCK = 256
GROUP = 8
WINDOW = 176
PACKED_ROWS = 1536


def gelu_norm(pre_act, gamma, beta):
    activated = jax.nn.gelu(pre_act, approximate=False)
    mean_val = jnp.mean(activated, axis=-1, keepdims=True)
    centered = activated - mean_val
    variance = jnp.mean(centered * centered, axis=-1, keepdims=True)
    return centered * lax.rsqrt(variance + LN_EPS) * gamma + beta


def over_rows(rows, unrolled, step, carry):
    full = rows // ROW_CHUNK
    if unrolled:
        for i in range(full):
            carry = step(i * ROW_CHUNK, ROW_CHUNK, carry)
    else:
        carry = lax.fori_loop(0, full, lambda i, c: step(pl.multiple_of(i * ROW_CHUNK, ROW_CHUNK), ROW_CHUNK, c), carry)
    if rows % ROW_CHUNK:
        carry = step(full * ROW_CHUNK, rows % ROW_CHUNK, carry)
    return carry


def params(**kw):
    return pltpu.CompilerParams(vmem_limit_bytes=VMEM_LIMIT, **kw)


def base_of(off_ref, g, slots):
    return pl.multiple_of(jnp.minimum(off_ref[g * GROUP] // 16, (slots - WINDOW) // 16) * 16, 16)


def pick_kernel(bounds_ref, off_ref, seat_ref, rowpos_ref, hid_ref, out_ref):
    k = pl.program_id(0)
    slots = out_ref.shape[0]
    depth, held = hid_ref.shape[0], rowpos_ref.shape[0]
    g = bounds_ref[0] + k

    @pl.when(k == 0)
    def _():
        out_ref[...] = jnp.zeros_like(out_ref)

    @pl.when(g < bounds_ref[1])
    def _():
        base = base_of(off_ref, g, slots)
        hot = (rowpos_ref[...] == lax.broadcasted_iota(jnp.int32, (held, depth), 1)).astype(jnp.bfloat16)
        move = (seat_ref[0] - base == lax.broadcasted_iota(jnp.int32, (WINDOW, held), 0)).astype(jnp.bfloat16)
        hot = jnp.dot(move, hot, preferred_element_type=jnp.float32).astype(jnp.bfloat16)
        got = jnp.dot(hot, hid_ref[...], preferred_element_type=jnp.float32)
        window = pl.ds(base, WINDOW)
        out_ref[window, :] = (out_ref[window, :].astype(jnp.float32) + got).astype(jnp.bfloat16)


def pick(hidden, rowpos_col, seat_row, bounds, offset, slots):
    groups = hidden.shape[0] // GROUP
    depth = GROUP * hidden.shape[1]
    width = hidden.shape[2]
    held = seat_row.shape[2]

    def at(k, bounds):
        return jnp.minimum(jnp.minimum(bounds[0] + k, bounds[1] - 1), groups - 1)

    return pl.pallas_call(
        pick_kernel,
        grid_spec=pltpu.PrefetchScalarGridSpec(
            num_scalar_prefetch=2,
            grid=(groups,),
            in_specs=[
                pl.BlockSpec((1, 1, held), lambda k, bounds, off: (at(k, bounds), 0, 0)),
                pl.BlockSpec((held, 1), lambda k, bounds, off: (at(k, bounds), 0)),
                pl.BlockSpec((depth, width), lambda k, bounds, off: (at(k, bounds), 0)),
            ],
            out_specs=pl.BlockSpec((slots, width), lambda k, bounds, off: (0, 0)),
        ),
        out_shape=jax.ShapeDtypeStruct((slots, width), jnp.bfloat16),
        compiler_params=params(),
        cost_estimate=pl.CostEstimate(flops=2 * WINDOW * groups * depth * width, bytes_accessed=hidden.size * 2, transcendentals=0),
        name="pick",
    )(bounds, offset, seat_row, rowpos_col, hidden.reshape(groups * depth, width))


def put_kernel(off_ref, seat_ref, rowpos_ref, dh_ref, out_ref):
    depth, held = out_ref.shape[0], seat_ref.shape[0]
    base = base_of(off_ref, pl.program_id(0), dh_ref.shape[0])
    move = (seat_ref[...] - base == lax.broadcasted_iota(jnp.int32, (held, WINDOW), 1)).astype(jnp.bfloat16)
    rows = dh_ref[pl.ds(base, WINDOW), :].astype(jnp.bfloat16)
    rows = jnp.dot(move, rows, preferred_element_type=jnp.float32).astype(jnp.bfloat16)
    hot = (rowpos_ref[0] == lax.broadcasted_iota(jnp.int32, (depth, held), 0)).astype(jnp.bfloat16)
    out_ref[...] = jnp.dot(hot, rows, preferred_element_type=jnp.float32).astype(jnp.bfloat16)


def put(d_rows, rowpos_row, seat_col, offset, batch, seq_len):
    groups = batch // GROUP
    depth = GROUP * seq_len
    slots, width = d_rows.shape
    held = rowpos_row.shape[2]
    out = pl.pallas_call(
        put_kernel,
        grid_spec=pltpu.PrefetchScalarGridSpec(
            num_scalar_prefetch=1,
            grid=(groups,),
            in_specs=[
                pl.BlockSpec((held, 1), lambda g, off: (g, 0)),
                pl.BlockSpec((1, 1, held), lambda g, off: (g, 0, 0)),
                pl.BlockSpec((slots, width), lambda g, off: (0, 0), pipeline_mode=pl.Buffered(1)),
            ],
            out_specs=pl.BlockSpec((depth, width), lambda g, off: (g, 0)),
        ),
        out_shape=jax.ShapeDtypeStruct((groups * depth, width), jnp.bfloat16),
        compiler_params=params(),
        cost_estimate=pl.CostEstimate(flops=2 * WINDOW * groups * depth * width, bytes_accessed=groups * depth * width * 2, transcendentals=0),
        name="put",
    )(offset, seat_col, rowpos_row, d_rows)
    return out.reshape(batch, seq_len, width)


def logits_kernel(unrolled, which_ref, t_ref, embed_ref, bias_ref, lab_ref, z_ref, stat_ref):
    del which_ref
    t_blk = t_ref[...].astype(jnp.bfloat16)
    lab = lab_ref[...]
    cols = t_blk.shape[0]

    def step(start, size, carry):
        top, total, target = carry
        rows = pl.ds(start, size)
        z = lax.dot_general(embed_ref[rows, :], t_blk, (((1,), (1,)), ((), ())), preferred_element_type=jnp.float32)
        z = z + bias_ref[rows, :]
        z_ref[rows, :] = z
        new_top = jnp.maximum(top, jnp.max(z, axis=0, keepdims=True))
        total = total * jnp.exp(top - new_top) + jnp.sum(jnp.exp(z - new_top), axis=0, keepdims=True)
        hot = lab - start == lax.broadcasted_iota(jnp.int32, (size, cols), 0)
        target = target + jnp.sum(jnp.where(hot, z, 0.0), axis=0, keepdims=True)
        return new_top, total, target

    zero = jnp.zeros((1, cols), jnp.float32)
    first = (jnp.full((1, cols), -jnp.inf, jnp.float32), zero, zero)
    top, total, target = over_rows(embed_ref.shape[0], unrolled, step, first)
    stat_ref[0:1, :] = top
    stat_ref[1:2, :] = total
    stat_ref[2:3, :] = target
    stat_ref[3:8, :] = jnp.zeros((5, cols), jnp.float32)


def block_map(planes, per_plane):
    if planes == 0:
        return lambda k, which: k
    return lambda k, which: lax.rem(which[0] + 1 + k // per_plane, planes) * per_plane + lax.rem(k, per_plane)


def logits_call(unrolled, which, t_rows, embed, bias_col, lab_row, planes, per_plane):
    slots = lab_row.shape[1]
    vocab, width = embed.shape
    where = block_map(planes, per_plane)
    return pl.pallas_call(
        functools.partial(logits_kernel, unrolled),
        grid_spec=pltpu.PrefetchScalarGridSpec(
            num_scalar_prefetch=1,
            grid=(slots // BLOCK_N,),
            in_specs=[
                pl.BlockSpec((BLOCK_N, width), lambda k, which: (where(k, which), 0)),
                pl.BlockSpec((vocab, width), lambda k, which: (0, 0), pipeline_mode=pl.Buffered(1)),
                pl.BlockSpec((vocab, 1), lambda k, which: (0, 0), pipeline_mode=pl.Buffered(1)),
                pl.BlockSpec((1, BLOCK_N), lambda k, which: (0, k)),
            ],
            out_specs=[
                pl.BlockSpec((vocab, BLOCK_N), lambda k, which: (0, k)),
                pl.BlockSpec((8, BLOCK_N), lambda k, which: (0, k)),
            ],
        ),
        out_shape=[jax.ShapeDtypeStruct((vocab, slots), jnp.float32), jax.ShapeDtypeStruct((8, slots), jnp.float32)],
        compiler_params=params(),
        cost_estimate=pl.CostEstimate(flops=2 * slots * vocab * width, bytes_accessed=slots * vocab * 4, transcendentals=slots * vocab),
        name="logits",
    )(which, t_rows, embed, bias_col, lab_row)


def dz_of(z, stat_ref, lab, start):
    soft = jnp.exp(z - stat_ref[0:1, :]) * stat_ref[1:2, :]
    hot = lab - start == lax.broadcasted_iota(jnp.int32, z.shape, 0)
    return jnp.where(hot, soft - 1.0, soft) * stat_ref[2:3, :]


def dt_kernel(unrolled, z_ref, stat_ref, lab_ref, embed_ref, dt_ref):
    lab = lab_ref[...]

    def step(start, size, acc):
        rows = pl.ds(start, size)
        dz = dz_of(z_ref[rows, :], stat_ref, lab, start).astype(jnp.bfloat16)
        return acc + lax.dot_general(dz, embed_ref[rows, :], (((0,), (0,)), ((), ())), preferred_element_type=jnp.float32)

    dt_ref[...] = over_rows(embed_ref.shape[0], unrolled, step, jnp.zeros(dt_ref.shape, jnp.float32))


def dt_call(unrolled, z, stat, lab_row, embed):
    slots = z.shape[1]
    vocab, width = embed.shape
    block = DT_BLOCK
    return pl.pallas_call(
        functools.partial(dt_kernel, unrolled),
        grid=(slots // block,),
        in_specs=[
            pl.BlockSpec((vocab, block), lambda k: (0, k)),
            pl.BlockSpec((8, block), lambda k: (0, k)),
            pl.BlockSpec((1, block), lambda k: (0, k)),
            pl.BlockSpec((vocab, width), lambda k: (0, 0), pipeline_mode=pl.Buffered(1)),
        ],
        out_specs=pl.BlockSpec((block, width), lambda k: (k, 0)),
        out_shape=jax.ShapeDtypeStruct((slots, width), jnp.float32),
        compiler_params=params(),
        cost_estimate=pl.CostEstimate(flops=2 * slots * vocab * width, bytes_accessed=slots * vocab * 4, transcendentals=slots * vocab),
        name="dt",
    )(z, stat, lab_row, embed)


def de_kernel(unrolled, first, part, which_ref, z_ref, stat_ref, lab_ref, t_ref, *rest):
    del which_ref
    if first:
        de_out, db_out, de_ref, db_ref, sems = rest
    else:
        de_in, db_in, de_out, db_out, de_ref, db_ref, sems = rest
    k = pl.program_id(0)
    part_rows = de_ref.shape[0]
    here = pl.ds(part * part_rows, part_rows)

    @pl.when(k == 0)
    def _():
        if first:
            de_ref[...] = jnp.zeros_like(de_ref)
            db_ref[...] = jnp.zeros_like(db_ref)
        else:
            one = pltpu.make_async_copy(de_in.at[here], de_ref, sems.at[0])
            two = pltpu.make_async_copy(db_in.at[here], db_ref, sems.at[1])
            one.start()
            two.start()
            one.wait()
            two.wait()

    lab = lab_ref[...] - part * part_rows
    t_blk = t_ref[...].astype(jnp.bfloat16)

    def step(start, size, carry):
        rows = pl.ds(start, size)
        dz = dz_of(z_ref[rows, :], stat_ref, lab, start)
        lanes = dz[:, 0:128]
        for c in range(128, dz.shape[1], 128):
            lanes = lanes + dz[:, c:c + 128]
        db_ref[rows, :] += lanes
        de_ref[rows, :] += jnp.dot(dz.astype(jnp.bfloat16), t_blk, preferred_element_type=jnp.float32)
        return carry

    over_rows(part_rows, unrolled, step, 0)

    @pl.when(k == pl.num_programs(0) - 1)
    def _():
        one = pltpu.make_async_copy(de_ref, de_out.at[here], sems.at[0])
        two = pltpu.make_async_copy(db_ref, db_out.at[here], sems.at[1])
        one.start()
        two.start()
        one.wait()
        two.wait()


def de_call(unrolled, which, z, stat, lab_row, t_rows, planes, per_plane, carry=None, part=0, parts=1):
    vocab, slots = z.shape
    width = t_rows.shape[1]
    where = block_map(planes, per_plane)
    first = carry is None
    part_rows = vocab // parts
    in_specs = [
        pl.BlockSpec((part_rows, BLOCK_N), lambda k, which: (part, k)),
        pl.BlockSpec((8, BLOCK_N), lambda k, which: (0, k)),
        pl.BlockSpec((1, BLOCK_N), lambda k, which: (0, k)),
        pl.BlockSpec((BLOCK_N, width), lambda k, which: (where(k, which), 0)),
    ]
    args = [which, z, stat, lab_row, t_rows]
    aliases = {}
    if not first:
        in_specs += [pl.BlockSpec(memory_space=pl.ANY), pl.BlockSpec(memory_space=pl.ANY)]
        args += list(carry)
        aliases = {5: 0, 6: 1}
    return pl.pallas_call(
        functools.partial(de_kernel, unrolled, first, part),
        grid_spec=pltpu.PrefetchScalarGridSpec(
            num_scalar_prefetch=1,
            grid=(slots // BLOCK_N,),
            in_specs=in_specs,
            out_specs=[pl.BlockSpec(memory_space=pl.ANY), pl.BlockSpec(memory_space=pl.ANY)],
            scratch_shapes=[pltpu.VMEM((part_rows, width), jnp.float32), pltpu.VMEM((part_rows, 128), jnp.float32), pltpu.SemaphoreType.DMA((2,))],
        ),
        out_shape=[jax.ShapeDtypeStruct((vocab, width), jnp.float32), jax.ShapeDtypeStruct((vocab, 128), jnp.float32)],
        input_output_aliases=aliases,
        compiler_params=params(),
        cost_estimate=pl.CostEstimate(flops=2 * slots * part_rows * width, bytes_accessed=slots * part_rows * 4, transcendentals=slots * part_rows),
        name="de",
    )(*args)


def combine(stat, weights_row, denom):
    parts = lax.all_gather(stat[:3], "tp", axis=0)
    top = jnp.max(parts[:, 0], axis=0)
    total = jnp.sum(parts[:, 1] * jnp.exp(parts[:, 0] - top[None]), axis=0)
    target = jnp.sum(parts[:, 2], axis=0)
    zero = jnp.zeros_like(top)
    rows = jnp.stack([top, 1.0 / total, weights_row / denom, zero, zero, zero, zero, zero])
    return rows, jnp.log(total) + top - target


def packed(values, index, slots):
    hot = index[..., None, :] == jnp.arange(slots, dtype=jnp.int32)[:, None]
    return jnp.sum(jnp.where(hot, values[..., None, :], 0), axis=-1)


def solution(mesh):
    dp, tp = mesh.shape["dp"], mesh.shape["tp"]

    def body(unrolled, slots, hidden, positions, weights, small, counts, w_t, b_t, gamma, beta, embed, out_bias):
        batch, seq_len, width = hidden.shape
        max_pred = positions.shape[1]
        shard_vocab = embed.shape[0]
        groups = batch // GROUP
        share = slots // tp
        per_plane = slots // BLOCK_N
        dp_idx, tp_idx = lax.axis_index("dp"), lax.axis_index("tp")
        which = dp_idx.reshape(1).astype(jnp.int32)
        denom = jnp.sum(counts).astype(jnp.float32) + LOSS_EPS

        column = jnp.arange(max_pred, dtype=jnp.int32)
        before = (jnp.arange(batch)[:, None] > jnp.arange(batch)[None, :]).astype(jnp.float32)
        by_seq = jnp.sum(weights, axis=1)
        offset = jnp.sum(before * by_seq[None, :], axis=1).astype(jnp.int32)
        seat = jnp.where(weights > 0, offset[:, None] + column, -WINDOW * batch)
        first_of = offset.reshape(groups, GROUP)[:, 0]
        ends = first_of + jnp.sum(by_seq.reshape(groups, GROUP), axis=1).astype(jnp.int32)
        row_of = positions + (jnp.arange(batch, dtype=jnp.int32) % GROUP * seq_len)[:, None]
        rowpos_col = row_of.reshape(-1, 1)
        seat_row = seat.reshape(groups, 1, -1)

        def transform(rows):
            pre_act = jnp.dot(rows, w_t, preferred_element_type=jnp.float32) + b_t
            return gelu_norm(pre_act, gamma, beta).astype(jnp.bfloat16)

        low = tp_idx * share
        bounds = jnp.sum(jnp.stack([ends <= low, first_of < low + share]).astype(jnp.int32), axis=1)
        some = pick(hidden, rowpos_col, seat_row, bounds, offset, slots)
        part_rows = lax.dynamic_slice_in_dim(some, low, share, 0)
        t_part = lax.optimization_barrier(transform(part_rows).astype(jnp.float32))
        t_all = lax.all_gather(t_part, ("dp", "tp"), axis=0, tiled=True)

        small, held, bias_col, t_part = lax.optimization_barrier((small, hidden, out_bias, t_part))
        bias_col = bias_col.reshape(-1, 1)
        every = jnp.array([0, groups], jnp.int32)
        tok_rows = pick(held, rowpos_col, seat_row, every, offset, slots)
        pre_act = jnp.dot(tok_rows, w_t, preferred_element_type=jnp.float32) + b_t
        normed, norm_vjp = jax.vjp(gelu_norm, pre_act, gamma, beta)
        t_own = normed.astype(jnp.bfloat16)

        turned = lax.dynamic_slice_in_dim(jnp.concatenate([small, small]), dp_idx, dp, 0)
        ahead = jnp.sum(jnp.where(before[None] > 0, jnp.sum(turned[:, 1].reshape(dp, 1, batch, max_pred), axis=3), 0.0), axis=2)
        index = jnp.where(turned[:, 1].reshape(dp, batch, max_pred) > 0, ahead[:, :, None].astype(jnp.int32) + column, -1)
        index = index.reshape(dp, batch * max_pred)
        labels = turned[:, 0].astype(jnp.int32) - tp_idx * shard_vocab
        total = jnp.sum(turned[:, 1], axis=1)
        weight_rows = (jnp.arange(slots, dtype=jnp.int32)[None, :] < total[:, None].astype(jnp.int32)).astype(jnp.float32)
        own_lab = packed(labels[:1], index[:1], slots)
        z_own, stat_own = logits_call(unrolled, which, t_own, embed, bias_col, own_lab, 0, per_plane)
        rows_own, ce = combine(stat_own, weight_rows[0], denom)
        dt_part = dt_call(unrolled, z_own, rows_own, own_lab, embed)
        d_normed = lax.psum(dt_part, "tp")
        carry = de_call(unrolled, which, z_own, rows_own, own_lab, t_own, 0, per_plane)
        far_lab = packed(labels[1:], index[1:], slots).reshape(1, -1)
        loss = jnp.sum(weight_rows[0] * ce)

        t_all, carry, far_lab = lax.optimization_barrier((t_all, carry, far_lab))
        z_far, stat_far = logits_call(unrolled, which, t_all, embed, bias_col, far_lab, dp, per_plane)
        rows_far, _ = combine(stat_far, weight_rows[1:].reshape(-1), denom)

        d_normed, rows_far = lax.optimization_barrier((d_normed, rows_far))
        d_pre, d_gamma, d_beta = norm_vjp(d_normed)
        d_pre_bf = d_pre.astype(jnp.bfloat16)
        d_rows = jnp.einsum("ne,de->nd", d_pre_bf, w_t, preferred_element_type=jnp.float32).astype(jnp.bfloat16)
        cut = width // tp
        part_cols = lax.dynamic_slice_in_dim(tok_rows, tp_idx * cut, cut, 1)
        d_w_t = jnp.einsum("nd,ne->de", part_cols, d_pre_bf, preferred_element_type=jnp.float32)
        vecs = [jnp.sum(d_pre, axis=0)[None], d_gamma[None], d_beta[None], jnp.full((5, width), loss)]
        block = jnp.concatenate([d_w_t] + vecs)
        d_rows, block, de_sum, db_sum = lax.optimization_barrier((d_rows, block, *carry))
        block = lax.psum(block, "dp")
        carry = de_call(unrolled, which, z_far, rows_far, far_lab, t_all, dp, per_plane, (de_sum, db_sum), 0, 2)
        block, de_sum, db_sum = lax.optimization_barrier((block, *carry))
        d_w_t = lax.all_gather(block[:cut], "tp", axis=0, tiled=True)
        d_embed, d_bias = de_call(unrolled, which, z_far, rows_far, far_lab, t_all, dp, per_plane, (de_sum, db_sum), 1, 2)
        d_rows, d_bias = lax.optimization_barrier((d_rows, d_bias))
        d_hidden = put(d_rows, row_of.reshape(groups, 1, -1), seat.reshape(-1, 1), offset, batch, seq_len)
        d_out_bias = jnp.sum(d_bias, axis=1)
        return block[cut + 3, 0] / denom, d_hidden, d_w_t, block[cut], block[cut + 1], block[cut + 2], d_embed, d_out_bias

    def local_step(hidden, positions, labels, weights, w_t, b_t, gamma, beta, embed, out_bias):
        small = jnp.stack([labels.reshape(-1).astype(jnp.float32), weights.reshape(-1)])
        small = lax.all_gather(small, "dp", axis=0)
        counts = jnp.sum((small[:, 1] > 0).astype(jnp.int32), axis=1)
        fits = jnp.max(counts) <= PACKED_ROWS
        args = (hidden, positions, weights, small, counts, w_t, b_t, gamma, beta, embed, out_bias)
        return lax.cond(fits, functools.partial(body, True, PACKED_ROWS), functools.partial(body, False, labels.size), *args)

    in_specs = (P("dp", None, None), P("dp", None), P("dp", None), P("dp", None), P(None, None), P(None), P(None), P(None), P("tp", None), P("tp"))
    out_specs = (P(), P("dp", None, None), P(None, None), P(None), P(None), P(None), P("tp", None), P("tp"))
    return jax.shard_map(local_step, mesh=mesh, in_specs=in_specs, out_specs=out_specs, check_vma=False)
```

```python
import functools

import jax
import jax.numpy as jnp
from jax import lax
from jax.experimental import pallas as pl
from jax.experimental.pallas import tpu as pltpu
from jax.sharding import PartitionSpec as P

LN_EPS = 1e-12
LOSS_EPS = 1e-5
VMEM_LIMIT = 60 * 1024 * 1024
ROW_CHUNK = 512
BLOCK_N = 512
DT_BLOCK = 256
GROUP = 8
WINDOW = 176
PACKED_ROWS = 1536


def gelu_norm(pre_act, gamma, beta):
    activated = jax.nn.gelu(pre_act, approximate=False)
    mean_val = jnp.mean(activated, axis=-1, keepdims=True)
    centered = activated - mean_val
    variance = jnp.mean(centered * centered, axis=-1, keepdims=True)
    return centered * lax.rsqrt(variance + LN_EPS) * gamma + beta


def two_stage(rows, make, use, carry):
    full, tail = rows // ROW_CHUNK, rows % ROW_CHUNK
    make(0, ROW_CHUNK, 0)

    def pair(i, carry):
        for half in range(2):
            start = pl.multiple_of(i * (2 * ROW_CHUNK) + half * ROW_CHUNK, ROW_CHUNK)
            make(start + ROW_CHUNK, ROW_CHUNK, 1 - half)
            carry = use(start, ROW_CHUNK, half, carry)
        return carry

    pairs = (full - 1) // 2
    carry = lax.fori_loop(0, pairs, pair, carry)
    for j in range(2 * pairs, full):
        if j + 1 < full:
            make((j + 1) * ROW_CHUNK, ROW_CHUNK, (j + 1) % 2)
        elif tail:
            make(full * ROW_CHUNK, tail, full % 2)
        carry = use(j * ROW_CHUNK, ROW_CHUNK, j % 2, carry)
    if tail:
        carry = use(full * ROW_CHUNK, tail, full % 2, carry)
    return carry


def params(**kw):
    return pltpu.CompilerParams(vmem_limit_bytes=VMEM_LIMIT, **kw)


def base_of(off_ref, g, slots):
    return pl.multiple_of(jnp.minimum(off_ref[g * GROUP] // 16, (slots - WINDOW) // 16) * 16, 16)


def pick_kernel(bounds_ref, off_ref, seat_ref, rowpos_ref, hid_ref, out_ref):
    k = pl.program_id(0)
    slots = out_ref.shape[0]
    depth, held = hid_ref.shape[0], rowpos_ref.shape[0]
    g = bounds_ref[0] + k

    @pl.when(k == 0)
    def _():
        out_ref[...] = jnp.zeros_like(out_ref)

    @pl.when(g < bounds_ref[1])
    def _():
        base = base_of(off_ref, g, slots)
        hot = (rowpos_ref[...] == lax.broadcasted_iota(jnp.int32, (held, depth), 1)).astype(jnp.bfloat16)
        move = (seat_ref[0] - base == lax.broadcasted_iota(jnp.int32, (WINDOW, held), 0)).astype(jnp.bfloat16)
        hot = jnp.dot(move, hot, preferred_element_type=jnp.float32).astype(jnp.bfloat16)
        got = jnp.dot(hot, hid_ref[...], preferred_element_type=jnp.float32)
        window = pl.ds(base, WINDOW)
        out_ref[window, :] = (out_ref[window, :].astype(jnp.float32) + got).astype(jnp.bfloat16)


def pick(hidden, rowpos_col, seat_row, bounds, offset, slots):
    groups = hidden.shape[0] // GROUP
    depth = GROUP * hidden.shape[1]
    width = hidden.shape[2]
    held = seat_row.shape[2]

    def at(k, bounds):
        return jnp.minimum(jnp.minimum(bounds[0] + k, bounds[1] - 1), groups - 1)

    return pl.pallas_call(
        pick_kernel,
        grid_spec=pltpu.PrefetchScalarGridSpec(
            num_scalar_prefetch=2,
            grid=(groups,),
            in_specs=[
                pl.BlockSpec((1, 1, held), lambda k, bounds, off: (at(k, bounds), 0, 0)),
                pl.BlockSpec((held, 1), lambda k, bounds, off: (at(k, bounds), 0)),
                pl.BlockSpec((depth, width), lambda k, bounds, off: (at(k, bounds), 0)),
            ],
            out_specs=pl.BlockSpec((slots, width), lambda k, bounds, off: (0, 0)),
        ),
        out_shape=jax.ShapeDtypeStruct((slots, width), jnp.bfloat16),
        compiler_params=params(),
        cost_estimate=pl.CostEstimate(flops=2 * WINDOW * groups * depth * width, bytes_accessed=hidden.size * 2, transcendentals=0),
        name="pick",
    )(bounds, offset, seat_row, rowpos_col, hidden.reshape(groups * depth, width))


def put_kernel(off_ref, seat_ref, rowpos_ref, dh_ref, out_ref):
    depth, held = out_ref.shape[0], seat_ref.shape[0]
    base = base_of(off_ref, pl.program_id(0), dh_ref.shape[0])
    move = (seat_ref[...] - base == lax.broadcasted_iota(jnp.int32, (held, WINDOW), 1)).astype(jnp.bfloat16)
    rows = dh_ref[pl.ds(base, WINDOW), :].astype(jnp.bfloat16)
    rows = jnp.dot(move, rows, preferred_element_type=jnp.float32).astype(jnp.bfloat16)
    hot = (rowpos_ref[0] == lax.broadcasted_iota(jnp.int32, (depth, held), 0)).astype(jnp.bfloat16)
    out_ref[...] = jnp.dot(hot, rows, preferred_element_type=jnp.float32).astype(jnp.bfloat16)


def put(d_rows, rowpos_row, seat_col, offset, batch, seq_len):
    groups = batch // GROUP
    depth = GROUP * seq_len
    slots, width = d_rows.shape
    held = rowpos_row.shape[2]
    out = pl.pallas_call(
        put_kernel,
        grid_spec=pltpu.PrefetchScalarGridSpec(
            num_scalar_prefetch=1,
            grid=(groups,),
            in_specs=[
                pl.BlockSpec((held, 1), lambda g, off: (g, 0)),
                pl.BlockSpec((1, 1, held), lambda g, off: (g, 0, 0)),
                pl.BlockSpec((slots, width), lambda g, off: (0, 0), pipeline_mode=pl.Buffered(1)),
            ],
            out_specs=pl.BlockSpec((depth, width), lambda g, off: (g, 0)),
        ),
        out_shape=jax.ShapeDtypeStruct((groups * depth, width), jnp.bfloat16),
        compiler_params=params(),
        cost_estimate=pl.CostEstimate(flops=2 * WINDOW * groups * depth * width, bytes_accessed=groups * depth * width * 2, transcendentals=0),
        name="put",
    )(offset, seat_col, rowpos_row, d_rows)
    return out.reshape(batch, seq_len, width)


def logits_kernel(which_ref, t_ref, embed_ref, bias_ref, lab_ref, z_ref, stat_ref, even_ref, odd_ref, t_scr):
    del which_ref
    t_scr[...] = t_ref[...].astype(jnp.bfloat16)
    lab = lab_ref[...]
    cols = t_scr.shape[0]
    held = (even_ref, odd_ref)

    def make(start, size, slot):
        rows = pl.ds(start, size)
        z = lax.dot_general(embed_ref[rows, :], t_scr[...], (((1,), (1,)), ((), ())), preferred_element_type=jnp.float32)
        z = z + bias_ref[rows, :]
        z_ref[rows, :] = z
        held[slot][0:size, :] = z

    def use(start, size, slot, carry):
        top, total, target = carry
        z = held[slot][0:size, :]
        new_top = jnp.maximum(top, jnp.max(z, axis=0, keepdims=True))
        total = total * jnp.exp(top - new_top) + jnp.sum(jnp.exp(z - new_top), axis=0, keepdims=True)
        hot = lab - start == lax.broadcasted_iota(jnp.int32, (size, cols), 0)
        target = target + jnp.sum(jnp.where(hot, z, 0.0), axis=0, keepdims=True)
        return new_top, total, target

    zero = jnp.zeros((1, cols), jnp.float32)
    first = (jnp.full((1, cols), -jnp.inf, jnp.float32), zero, zero)
    top, total, target = two_stage(embed_ref.shape[0], make, use, first)
    stat_ref[0:1, :] = top
    stat_ref[1:2, :] = total
    stat_ref[2:3, :] = target
    stat_ref[3:8, :] = jnp.zeros((5, cols), jnp.float32)


def block_map(planes, per_plane):
    if planes == 0:
        return lambda k, which: k
    return lambda k, which: lax.rem(which[0] + 1 + k // per_plane, planes) * per_plane + lax.rem(k, per_plane)


def logits_call(which, t_rows, embed, bias_col, lab_row, planes, per_plane):
    slots = lab_row.shape[1]
    vocab, width = embed.shape
    where = block_map(planes, per_plane)
    return pl.pallas_call(
        logits_kernel,
        grid_spec=pltpu.PrefetchScalarGridSpec(
            num_scalar_prefetch=1,
            grid=(slots // BLOCK_N,),
            in_specs=[
                pl.BlockSpec((BLOCK_N, width), lambda k, which: (where(k, which), 0)),
                pl.BlockSpec((vocab, width), lambda k, which: (0, 0), pipeline_mode=pl.Buffered(1)),
                pl.BlockSpec((vocab, 1), lambda k, which: (0, 0), pipeline_mode=pl.Buffered(1)),
                pl.BlockSpec((1, BLOCK_N), lambda k, which: (0, k)),
            ],
            out_specs=[
                pl.BlockSpec((vocab, BLOCK_N), lambda k, which: (0, k)),
                pl.BlockSpec((8, BLOCK_N), lambda k, which: (0, k)),
            ],
            scratch_shapes=[pltpu.VMEM((ROW_CHUNK, BLOCK_N), jnp.float32)] * 2 + [pltpu.VMEM((BLOCK_N, width), jnp.bfloat16)],
        ),
        out_shape=[jax.ShapeDtypeStruct((vocab, slots), jnp.float32), jax.ShapeDtypeStruct((8, slots), jnp.float32)],
        compiler_params=params(),
        cost_estimate=pl.CostEstimate(flops=2 * slots * vocab * width, bytes_accessed=slots * vocab * 4, transcendentals=slots * vocab),
        name="logits",
    )(which, t_rows, embed, bias_col, lab_row)


def dz_of(z, stat_ref, lab, start):
    soft = jnp.exp(z - stat_ref[0:1, :]) * stat_ref[1:2, :]
    hot = lab - start == lax.broadcasted_iota(jnp.int32, z.shape, 0)
    return jnp.where(hot, soft - 1.0, soft) * stat_ref[2:3, :]


def dt_kernel(z_ref, stat_ref, lab_ref, embed_ref, dt_ref, even_ref, odd_ref):
    lab = lab_ref[...]
    held = (even_ref, odd_ref)
    dt_ref[...] = jnp.zeros_like(dt_ref)

    def make(start, size, slot):
        held[slot][0:size, :] = dz_of(z_ref[pl.ds(start, size), :], stat_ref, lab, start).astype(jnp.bfloat16)

    def use(start, size, slot, carry):
        dt_ref[...] += lax.dot_general(held[slot][0:size, :], embed_ref[pl.ds(start, size), :], (((0,), (0,)), ((), ())), preferred_element_type=jnp.float32)
        return carry

    two_stage(embed_ref.shape[0], make, use, 0)


def dt_call(z, stat, lab_row, embed):
    slots = z.shape[1]
    vocab, width = embed.shape
    block = DT_BLOCK
    return pl.pallas_call(
        dt_kernel,
        grid=(slots // block,),
        in_specs=[
            pl.BlockSpec((vocab, block), lambda k: (0, k)),
            pl.BlockSpec((8, block), lambda k: (0, k)),
            pl.BlockSpec((1, block), lambda k: (0, k)),
            pl.BlockSpec((vocab, width), lambda k: (0, 0), pipeline_mode=pl.Buffered(1)),
        ],
        out_specs=pl.BlockSpec((block, width), lambda k: (k, 0)),
        out_shape=jax.ShapeDtypeStruct((slots, width), jnp.float32),
        scratch_shapes=[pltpu.VMEM((ROW_CHUNK, block), jnp.bfloat16)] * 2,
        compiler_params=params(),
        cost_estimate=pl.CostEstimate(flops=2 * slots * vocab * width, bytes_accessed=slots * vocab * 4, transcendentals=slots * vocab),
        name="dt",
    )(z, stat, lab_row, embed)


def de_kernel(first, part, which_ref, z_ref, stat_ref, lab_ref, t_ref, *rest):
    del which_ref
    if first:
        de_out, db_out, de_ref, db_ref, t_scr, even_ref, odd_ref, sems = rest
    else:
        de_in, db_in, de_out, db_out, de_ref, db_ref, t_scr, even_ref, odd_ref, sems = rest
    k = pl.program_id(0)
    part_rows = de_ref.shape[0]
    here = pl.ds(part * part_rows, part_rows)

    @pl.when(k == 0)
    def _():
        if first:
            de_ref[...] = jnp.zeros_like(de_ref)
            db_ref[...] = jnp.zeros_like(db_ref)
        else:
            one = pltpu.make_async_copy(de_in.at[here], de_ref, sems.at[0])
            two = pltpu.make_async_copy(db_in.at[here], db_ref, sems.at[1])
            one.start()
            two.start()
            one.wait()
            two.wait()

    lab = lab_ref[...] - part * part_rows
    t_scr[...] = t_ref[...].astype(jnp.bfloat16)
    held = (even_ref, odd_ref)

    def make(start, size, slot):
        rows = pl.ds(start, size)
        dz = dz_of(z_ref[rows, :], stat_ref, lab, start)
        lanes = dz[:, 0:128]
        for c in range(128, dz.shape[1], 128):
            lanes = lanes + dz[:, c:c + 128]
        db_ref[rows, :] += lanes
        held[slot][0:size, :] = dz.astype(jnp.bfloat16)

    def use(start, size, slot, carry):
        de_ref[pl.ds(start, size), :] += jnp.dot(held[slot][0:size, :], t_scr[...], preferred_element_type=jnp.float32)
        return carry

    two_stage(part_rows, make, use, 0)

    @pl.when(k == pl.num_programs(0) - 1)
    def _():
        one = pltpu.make_async_copy(de_ref, de_out.at[here], sems.at[0])
        two = pltpu.make_async_copy(db_ref, db_out.at[here], sems.at[1])
        one.start()
        two.start()
        one.wait()
        two.wait()


def de_call(which, z, stat, lab_row, t_rows, planes, per_plane, carry=None, part=0, parts=1):
    vocab, slots = z.shape
    width = t_rows.shape[1]
    where = block_map(planes, per_plane)
    first = carry is None
    part_rows = vocab // parts
    in_specs = [
        pl.BlockSpec((part_rows, BLOCK_N), lambda k, which: (part, k)),
        pl.BlockSpec((8, BLOCK_N), lambda k, which: (0, k)),
        pl.BlockSpec((1, BLOCK_N), lambda k, which: (0, k)),
        pl.BlockSpec((BLOCK_N, width), lambda k, which: (where(k, which), 0)),
    ]
    args = [which, z, stat, lab_row, t_rows]
    aliases = {}
    if not first:
        in_specs += [pl.BlockSpec(memory_space=pl.ANY), pl.BlockSpec(memory_space=pl.ANY)]
        args += list(carry)
        aliases = {5: 0, 6: 1}
    return pl.pallas_call(
        functools.partial(de_kernel, first, part),
        grid_spec=pltpu.PrefetchScalarGridSpec(
            num_scalar_prefetch=1,
            grid=(slots // BLOCK_N,),
            in_specs=in_specs,
            out_specs=[pl.BlockSpec(memory_space=pl.ANY), pl.BlockSpec(memory_space=pl.ANY)],
            scratch_shapes=[pltpu.VMEM((part_rows, width), jnp.float32), pltpu.VMEM((part_rows, 128), jnp.float32), pltpu.VMEM((BLOCK_N, width), jnp.bfloat16)]
            + [pltpu.VMEM((ROW_CHUNK, BLOCK_N), jnp.bfloat16)] * 2
            + [pltpu.SemaphoreType.DMA((2,))],
        ),
        out_shape=[jax.ShapeDtypeStruct((vocab, width), jnp.float32), jax.ShapeDtypeStruct((vocab, 128), jnp.float32)],
        input_output_aliases=aliases,
        compiler_params=params(),
        cost_estimate=pl.CostEstimate(flops=2 * slots * part_rows * width, bytes_accessed=slots * part_rows * 4, transcendentals=slots * part_rows),
        name="de",
    )(*args)


def combine(stat, weights_row, denom):
    parts = lax.all_gather(stat[:3], "tp", axis=0)
    top = jnp.max(parts[:, 0], axis=0)
    total = jnp.sum(parts[:, 1] * jnp.exp(parts[:, 0] - top[None]), axis=0)
    target = jnp.sum(parts[:, 2], axis=0)
    zero = jnp.zeros_like(top)
    rows = jnp.stack([top, 1.0 / total, weights_row / denom, zero, zero, zero, zero, zero])
    return rows, jnp.log(total) + top - target


def packed(values, index, slots):
    hot = index[..., None, :] == jnp.arange(slots, dtype=jnp.int32)[:, None]
    return jnp.sum(jnp.where(hot, values[..., None, :], 0), axis=-1)


def earlier_of(batch):
    return (jnp.arange(batch)[:, None] > jnp.arange(batch)[None, :]).astype(jnp.float32)


def solution(mesh):
    dp, tp = mesh.shape["dp"], mesh.shape["tp"]

    def share_of(slots, hidden, weights, plan, w_t, b_t, gamma, beta):
        offset, _, _, rowpos_col, seat_row = plan
        share = slots // tp
        low = lax.axis_index("tp") * share
        groups = hidden.shape[0] // GROUP
        first_of = offset.reshape(groups, GROUP)[:, 0]
        ends = first_of + jnp.sum(weights.reshape(groups, -1), axis=1).astype(jnp.int32)
        bounds = jnp.sum(jnp.stack([ends <= low, first_of < low + share]).astype(jnp.int32), axis=1)
        some = pick(hidden, rowpos_col, seat_row, bounds, offset, slots)
        part_rows = lax.dynamic_slice_in_dim(some, low, share, 0)
        pre_act = jnp.dot(part_rows, w_t, preferred_element_type=jnp.float32) + b_t
        return lax.optimization_barrier(gelu_norm(pre_act, gamma, beta).astype(jnp.bfloat16).astype(jnp.float32))

    def body(slots, sent, hidden, positions, weights, turned, plan, w_t, b_t, gamma, beta, embed, out_bias):
        batch, seq_len, width = hidden.shape
        max_pred = positions.shape[1]
        shard_vocab = embed.shape[0]
        groups = batch // GROUP
        per_plane = slots // BLOCK_N
        dp_idx, tp_idx = lax.axis_index("dp"), lax.axis_index("tp")
        which = dp_idx.reshape(1).astype(jnp.int32)
        denom = jnp.sum(turned[:, 1]) + LOSS_EPS
        offset, seat, row_of, rowpos_col, seat_row = plan
        before, column = earlier_of(batch), jnp.arange(max_pred, dtype=jnp.int32)

        t_part = share_of(slots, hidden, weights, plan, w_t, b_t, gamma, beta) if sent is None else sent
        t_all = lax.all_gather(t_part, ("dp", "tp"), axis=0, tiled=True)

        turned, held, bias_col, t_part = lax.optimization_barrier((turned, hidden, out_bias, t_part))
        bias_col = bias_col.reshape(-1, 1)
        every = jnp.array([0, groups], jnp.int32)
        tok_rows = pick(held, rowpos_col, seat_row, every, offset, slots)
        pre_act = jnp.dot(tok_rows, w_t, preferred_element_type=jnp.float32) + b_t
        activated, gelu_vjp = jax.vjp(lambda u: jax.nn.gelu(u, approximate=False), pre_act)
        slope = gelu_vjp(jnp.ones_like(pre_act))[0]
        centered = activated - jnp.mean(activated, axis=-1, keepdims=True)
        spread = lax.rsqrt(jnp.mean(centered * centered, axis=-1, keepdims=True) + LN_EPS)
        unit = centered * spread
        t_own = (unit * gamma + beta).astype(jnp.bfloat16)
        slope, unit = lax.optimization_barrier((slope, unit))

        ahead = jnp.sum(jnp.where(before[None] > 0, jnp.sum(turned[:, 1].reshape(dp, 1, batch, max_pred), axis=3), 0.0), axis=2)
        index = jnp.where(turned[:, 1].reshape(dp, batch, max_pred) > 0, ahead[:, :, None].astype(jnp.int32) + column, -1)
        index = index.reshape(dp, batch * max_pred)
        labels = turned[:, 0].astype(jnp.int32) - tp_idx * shard_vocab
        total = jnp.sum(turned[:, 1], axis=1)
        weight_rows = (jnp.arange(slots, dtype=jnp.int32)[None, :] < total[:, None].astype(jnp.int32)).astype(jnp.float32)
        own_lab = packed(labels[:1], index[:1], slots)
        z_own, stat_own = logits_call(which, t_own, embed, bias_col, own_lab, 0, per_plane)
        rows_own, ce = combine(stat_own, weight_rows[0], denom)
        dt_part = dt_call(z_own, rows_own, own_lab, embed)
        d_normed = lax.psum(dt_part, "tp")
        carry = de_call(which, z_own, rows_own, own_lab, t_own, 0, per_plane)
        far_lab = packed(labels[1:], index[1:], slots).reshape(1, -1)
        loss = jnp.sum(weight_rows[0] * ce)

        t_all, carry, far_lab = lax.optimization_barrier((t_all, carry, far_lab))
        z_far, stat_far = logits_call(which, t_all, embed, bias_col, far_lab, dp, per_plane)
        rows_far, _ = combine(stat_far, weight_rows[1:].reshape(-1), denom)

        de_sum, db_sum = de_call(which, z_far, rows_far, far_lab, t_all, dp, per_plane, carry)

        d_normed, db_sum = lax.optimization_barrier((d_normed, db_sum))
        d_unit = d_normed * gamma
        along = jnp.mean(d_unit * unit, axis=-1, keepdims=True)
        d_act = (d_unit - jnp.mean(d_unit, axis=-1, keepdims=True) - unit * along) * spread
        d_pre = d_act * slope
        d_gamma = jnp.sum(d_normed * unit, axis=0)
        d_beta = jnp.sum(d_normed, axis=0)
        d_pre_bf = d_pre.astype(jnp.bfloat16)
        cut = width // tp
        part_cols = lax.dynamic_slice_in_dim(tok_rows, tp_idx * cut, cut, 1)
        d_w_t = jnp.einsum("nd,ne->de", part_cols, d_pre_bf, preferred_element_type=jnp.float32)
        vecs = [jnp.sum(d_pre, axis=0)[None], d_gamma[None], d_beta[None], jnp.full((5, width), loss)]
        block, d_pre_bf = lax.optimization_barrier((jnp.concatenate([d_w_t] + vecs), d_pre_bf))
        block = lax.psum(block, "dp")
        d_w_t = lax.all_gather(block[:cut], "tp", axis=0, tiled=True)
        d_rows = jnp.einsum("ne,de->nd", d_pre_bf, w_t, preferred_element_type=jnp.float32).astype(jnp.bfloat16)
        d_hidden = put(d_rows, row_of.reshape(groups, 1, -1), seat.reshape(-1, 1), offset, batch, seq_len)
        d_out_bias = jnp.sum(db_sum, axis=1)
        return block[cut + 3, 0] / denom, d_hidden, d_w_t, block[cut], block[cut + 1], block[cut + 2], de_sum, d_out_bias

    def local_step(hidden, positions, labels, weights, w_t, b_t, gamma, beta, embed, out_bias):
        batch, seq_len, _ = hidden.shape
        groups = batch // GROUP
        small = jnp.stack([labels.reshape(-1).astype(jnp.float32), weights.reshape(-1)])
        rings = [[((j + k) % dp, j) for j in range(dp)] for k in range(1, dp)]
        turned = jnp.stack([small] + [lax.ppermute(small, "dp", ring) for ring in rings])

        column = jnp.arange(weights.shape[1], dtype=jnp.int32)
        by_seq = jnp.sum(weights, axis=1)
        offset = jnp.sum(earlier_of(batch) * by_seq[None, :], axis=1).astype(jnp.int32)
        seat = jnp.where(weights > 0, offset[:, None] + column, -WINDOW * batch)
        row_of = positions + (jnp.arange(batch, dtype=jnp.int32) % GROUP * seq_len)[:, None]
        plan = (offset, seat, row_of, row_of.reshape(-1, 1), seat.reshape(groups, 1, -1))
        sent = share_of(PACKED_ROWS, hidden, weights, plan, w_t, b_t, gamma, beta)
        fits = jnp.max(jnp.sum(turned[:, 1], axis=1)) <= PACKED_ROWS
        args = (hidden, positions, weights, turned, plan, w_t, b_t, gamma, beta, embed, out_bias)

        def packed_form(sent, *args):
            return body(PACKED_ROWS, sent, *args)

        def whole_form(sent, *args):
            return body(labels.size, None, *args)

        return lax.cond(fits, packed_form, whole_form, sent, *args)

    in_specs = (P("dp", None, None), P("dp", None), P("dp", None), P("dp", None), P(None, None), P(None), P(None), P(None), P("tp", None), P("tp"))
    out_specs = (P(), P("dp", None, None), P(None, None), P(None), P(None), P(None), P("tp", None), P("tp"))
    return jax.shard_map(local_step, mesh=mesh, in_specs=in_specs, out_specs=out_specs, check_vma=False)
```

```python
import functools

import jax
import jax.numpy as jnp
from jax import lax
from jax.experimental import pallas as pl
from jax.experimental.pallas import tpu as pltpu
from jax.sharding import PartitionSpec as P

LN_EPS = 1e-12
LOSS_EPS = 1e-5
VMEM_LIMIT = 60 * 1024 * 1024
ROW_CHUNK = 512
BLOCK_N = 512
DT_BLOCK = 256
GROUP = 8
WINDOW = 176
PACKED_ROWS = 1536


def gelu_norm(pre_act, gamma, beta):
    activated = jax.nn.gelu(pre_act, approximate=False)
    mean_val = jnp.mean(activated, axis=-1, keepdims=True)
    centered = activated - mean_val
    variance = jnp.mean(centered * centered, axis=-1, keepdims=True)
    return centered * lax.rsqrt(variance + LN_EPS) * gamma + beta


def over_rows(rows, unrolled, step, carry):
    full = rows // ROW_CHUNK
    if unrolled:
        for i in range(full):
            carry = step(i * ROW_CHUNK, ROW_CHUNK, carry)
    else:
        carry = lax.fori_loop(0, full, lambda i, c: step(pl.multiple_of(i * ROW_CHUNK, ROW_CHUNK), ROW_CHUNK, c), carry)
    if rows % ROW_CHUNK:
        carry = step(full * ROW_CHUNK, rows % ROW_CHUNK, carry)
    return carry


def params(**kw):
    return pltpu.CompilerParams(vmem_limit_bytes=VMEM_LIMIT, **kw)


def base_of(off_ref, g, slots):
    return pl.multiple_of(jnp.minimum(off_ref[g * GROUP] // 16, (slots - WINDOW) // 16) * 16, 16)


def pick_kernel(bounds_ref, off_ref, seat_ref, rowpos_ref, hid_ref, out_ref):
    k = pl.program_id(0)
    slots = out_ref.shape[0]
    depth, held = hid_ref.shape[0], rowpos_ref.shape[0]
    g = bounds_ref[0] + k

    @pl.when(k == 0)
    def _():
        out_ref[...] = jnp.zeros_like(out_ref)

    @pl.when(g < bounds_ref[1])
    def _():
        base = base_of(off_ref, g, slots)
        hot = (rowpos_ref[...] == lax.broadcasted_iota(jnp.int32, (held, depth), 1)).astype(jnp.bfloat16)
        move = (seat_ref[0] - base == lax.broadcasted_iota(jnp.int32, (WINDOW, held), 0)).astype(jnp.bfloat16)
        hot = jnp.dot(move, hot, preferred_element_type=jnp.float32).astype(jnp.bfloat16)
        got = jnp.dot(hot, hid_ref[...], preferred_element_type=jnp.float32)
        window = pl.ds(base, WINDOW)
        out_ref[window, :] = (out_ref[window, :].astype(jnp.float32) + got).astype(jnp.bfloat16)


def pick(hidden, rowpos_col, seat_row, bounds, offset, slots):
    groups = hidden.shape[0] // GROUP
    depth = GROUP * hidden.shape[1]
    width = hidden.shape[2]
    held = seat_row.shape[2]

    def at(k, bounds):
        return jnp.minimum(jnp.minimum(bounds[0] + k, bounds[1] - 1), groups - 1)

    return pl.pallas_call(
        pick_kernel,
        grid_spec=pltpu.PrefetchScalarGridSpec(
            num_scalar_prefetch=2,
            grid=(groups,),
            in_specs=[
                pl.BlockSpec((1, 1, held), lambda k, bounds, off: (at(k, bounds), 0, 0)),
                pl.BlockSpec((held, 1), lambda k, bounds, off: (at(k, bounds), 0)),
                pl.BlockSpec((depth, width), lambda k, bounds, off: (at(k, bounds), 0)),
            ],
            out_specs=pl.BlockSpec((slots, width), lambda k, bounds, off: (0, 0)),
        ),
        out_shape=jax.ShapeDtypeStruct((slots, width), jnp.bfloat16),
        compiler_params=params(),
        cost_estimate=pl.CostEstimate(flops=2 * WINDOW * groups * depth * width, bytes_accessed=hidden.size * 2, transcendentals=0),
        name="pick",
    )(bounds, offset, seat_row, rowpos_col, hidden.reshape(groups * depth, width))


def put_kernel(off_ref, seat_ref, rowpos_ref, dh_ref, out_ref):
    depth, held = out_ref.shape[0], seat_ref.shape[0]
    base = base_of(off_ref, pl.program_id(0), dh_ref.shape[0])
    move = (seat_ref[...] - base == lax.broadcasted_iota(jnp.int32, (held, WINDOW), 1)).astype(jnp.bfloat16)
    rows = dh_ref[pl.ds(base, WINDOW), :].astype(jnp.bfloat16)
    rows = jnp.dot(move, rows, preferred_element_type=jnp.float32).astype(jnp.bfloat16)
    hot = (rowpos_ref[0] == lax.broadcasted_iota(jnp.int32, (depth, held), 0)).astype(jnp.bfloat16)
    out_ref[...] = jnp.dot(hot, rows, preferred_element_type=jnp.float32).astype(jnp.bfloat16)


def put(d_rows, rowpos_row, seat_col, offset, batch, seq_len):
    groups = batch // GROUP
    depth = GROUP * seq_len
    slots, width = d_rows.shape
    held = rowpos_row.shape[2]
    out = pl.pallas_call(
        put_kernel,
        grid_spec=pltpu.PrefetchScalarGridSpec(
            num_scalar_prefetch=1,
            grid=(groups,),
            in_specs=[
                pl.BlockSpec((held, 1), lambda g, off: (g, 0)),
                pl.BlockSpec((1, 1, held), lambda g, off: (g, 0, 0)),
                pl.BlockSpec((slots, width), lambda g, off: (0, 0), pipeline_mode=pl.Buffered(1)),
            ],
            out_specs=pl.BlockSpec((depth, width), lambda g, off: (g, 0)),
        ),
        out_shape=jax.ShapeDtypeStruct((groups * depth, width), jnp.bfloat16),
        compiler_params=params(),
        cost_estimate=pl.CostEstimate(flops=2 * WINDOW * groups * depth * width, bytes_accessed=groups * depth * width * 2, transcendentals=0),
        name="put",
    )(offset, seat_col, rowpos_row, d_rows)
    return out.reshape(batch, seq_len, width)


def logits_kernel(unrolled, which_ref, t_ref, embed_ref, bias_ref, lab_ref, z_ref, stat_ref):
    del which_ref
    t_blk = t_ref[...].astype(jnp.bfloat16)
    lab = lab_ref[...]
    cols = t_blk.shape[0]

    def step(start, size, carry):
        top, total, target = carry
        rows = pl.ds(start, size)
        z = lax.dot_general(embed_ref[rows, :], t_blk, (((1,), (1,)), ((), ())), preferred_element_type=jnp.float32)
        z = z + bias_ref[rows, :]
        z_ref[rows, :] = z
        new_top = jnp.maximum(top, jnp.max(z, axis=0, keepdims=True))
        total = total * jnp.exp(top - new_top) + jnp.sum(jnp.exp(z - new_top), axis=0, keepdims=True)
        hot = lab - start == lax.broadcasted_iota(jnp.int32, (size, cols), 0)
        target = target + jnp.sum(jnp.where(hot, z, 0.0), axis=0, keepdims=True)
        return new_top, total, target

    zero = jnp.zeros((1, cols), jnp.float32)
    first = (jnp.full((1, cols), -jnp.inf, jnp.float32), zero, zero)
    top, total, target = over_rows(embed_ref.shape[0], unrolled, step, first)
    stat_ref[0:1, :] = top
    stat_ref[1:2, :] = total
    stat_ref[2:3, :] = target
    stat_ref[3:8, :] = jnp.zeros((5, cols), jnp.float32)


def block_map(planes, per_plane):
    if planes == 0:
        return lambda k, which: k
    return lambda k, which: lax.rem(which[0] + 1 + k // per_plane, planes) * per_plane + lax.rem(k, per_plane)


def logits_call(unrolled, which, t_rows, embed, bias_col, lab_row, planes, per_plane):
    slots = lab_row.shape[1]
    vocab, width = embed.shape
    where = block_map(planes, per_plane)
    return pl.pallas_call(
        functools.partial(logits_kernel, unrolled),
        grid_spec=pltpu.PrefetchScalarGridSpec(
            num_scalar_prefetch=1,
            grid=(slots // BLOCK_N,),
            in_specs=[
                pl.BlockSpec((BLOCK_N, width), lambda k, which: (where(k, which), 0)),
                pl.BlockSpec((vocab, width), lambda k, which: (0, 0), pipeline_mode=pl.Buffered(1)),
                pl.BlockSpec((vocab, 1), lambda k, which: (0, 0), pipeline_mode=pl.Buffered(1)),
                pl.BlockSpec((1, BLOCK_N), lambda k, which: (0, k)),
            ],
            out_specs=[
                pl.BlockSpec((vocab, BLOCK_N), lambda k, which: (0, k)),
                pl.BlockSpec((8, BLOCK_N), lambda k, which: (0, k)),
            ],
        ),
        out_shape=[jax.ShapeDtypeStruct((vocab, slots), jnp.float32), jax.ShapeDtypeStruct((8, slots), jnp.float32)],
        compiler_params=params(),
        cost_estimate=pl.CostEstimate(flops=2 * slots * vocab * width, bytes_accessed=slots * vocab * 4, transcendentals=slots * vocab),
        name="logits",
    )(which, t_rows, embed, bias_col, lab_row)


def dz_of(z, stat_ref, lab, start):
    soft = jnp.exp(z - stat_ref[0:1, :]) * stat_ref[1:2, :]
    hot = lab - start == lax.broadcasted_iota(jnp.int32, z.shape, 0)
    return jnp.where(hot, soft - 1.0, soft) * stat_ref[2:3, :]


def dt_kernel(unrolled, z_ref, stat_ref, lab_ref, embed_ref, dt_ref):
    lab = lab_ref[...]

    def step(start, size, acc):
        rows = pl.ds(start, size)
        dz = dz_of(z_ref[rows, :], stat_ref, lab, start).astype(jnp.bfloat16)
        return acc + lax.dot_general(dz, embed_ref[rows, :], (((0,), (0,)), ((), ())), preferred_element_type=jnp.float32)

    dt_ref[...] = over_rows(embed_ref.shape[0], unrolled, step, jnp.zeros(dt_ref.shape, jnp.float32))


def dt_call(unrolled, z, stat, lab_row, embed):
    slots = z.shape[1]
    vocab, width = embed.shape
    block = DT_BLOCK
    return pl.pallas_call(
        functools.partial(dt_kernel, unrolled),
        grid=(slots // block,),
        in_specs=[
            pl.BlockSpec((vocab, block), lambda k: (0, k)),
            pl.BlockSpec((8, block), lambda k: (0, k)),
            pl.BlockSpec((1, block), lambda k: (0, k)),
            pl.BlockSpec((vocab, width), lambda k: (0, 0), pipeline_mode=pl.Buffered(1)),
        ],
        out_specs=pl.BlockSpec((block, width), lambda k: (k, 0)),
        out_shape=jax.ShapeDtypeStruct((slots, width), jnp.float32),
        compiler_params=params(),
        cost_estimate=pl.CostEstimate(flops=2 * slots * vocab * width, bytes_accessed=slots * vocab * 4, transcendentals=slots * vocab),
        name="dt",
    )(z, stat, lab_row, embed)


def de_kernel(unrolled, first, part, which_ref, z_ref, stat_ref, lab_ref, t_ref, *rest):
    del which_ref
    if first:
        de_out, db_out, de_ref, db_ref, sems = rest
    else:
        de_in, db_in, de_out, db_out, de_ref, db_ref, sems = rest
    k = pl.program_id(0)
    part_rows = de_ref.shape[0]
    here = pl.ds(part * part_rows, part_rows)

    @pl.when(k == 0)
    def _():
        if first:
            de_ref[...] = jnp.zeros_like(de_ref)
            db_ref[...] = jnp.zeros_like(db_ref)
        else:
            one = pltpu.make_async_copy(de_in.at[here], de_ref, sems.at[0])
            two = pltpu.make_async_copy(db_in.at[here], db_ref, sems.at[1])
            one.start()
            two.start()
            one.wait()
            two.wait()

    lab = lab_ref[...] - part * part_rows
    t_blk = t_ref[...].astype(jnp.bfloat16)

    def step(start, size, carry):
        rows = pl.ds(start, size)
        dz = dz_of(z_ref[rows, :], stat_ref, lab, start)
        lanes = dz[:, 0:128]
        for c in range(128, dz.shape[1], 128):
            lanes = lanes + dz[:, c:c + 128]
        db_ref[rows, :] += lanes
        de_ref[rows, :] += jnp.dot(dz.astype(jnp.bfloat16), t_blk, preferred_element_type=jnp.float32)
        return carry

    over_rows(part_rows, unrolled, step, 0)

    @pl.when(k == pl.num_programs(0) - 1)
    def _():
        one = pltpu.make_async_copy(de_ref, de_out.at[here], sems.at[0])
        two = pltpu.make_async_copy(db_ref, db_out.at[here], sems.at[1])
        one.start()
        two.start()
        one.wait()
        two.wait()


def de_call(unrolled, which, z, stat, lab_row, t_rows, planes, per_plane, carry=None, part=0, parts=1):
    vocab, slots = z.shape
    width = t_rows.shape[1]
    where = block_map(planes, per_plane)
    first = carry is None
    part_rows = vocab // parts
    in_specs = [
        pl.BlockSpec((part_rows, BLOCK_N), lambda k, which: (part, k)),
        pl.BlockSpec((8, BLOCK_N), lambda k, which: (0, k)),
        pl.BlockSpec((1, BLOCK_N), lambda k, which: (0, k)),
        pl.BlockSpec((BLOCK_N, width), lambda k, which: (where(k, which), 0)),
    ]
    args = [which, z, stat, lab_row, t_rows]
    aliases = {}
    if not first:
        in_specs += [pl.BlockSpec(memory_space=pl.ANY), pl.BlockSpec(memory_space=pl.ANY)]
        args += list(carry)
        aliases = {5: 0, 6: 1}
    return pl.pallas_call(
        functools.partial(de_kernel, unrolled, first, part),
        grid_spec=pltpu.PrefetchScalarGridSpec(
            num_scalar_prefetch=1,
            grid=(slots // BLOCK_N,),
            in_specs=in_specs,
            out_specs=[pl.BlockSpec(memory_space=pl.ANY), pl.BlockSpec(memory_space=pl.ANY)],
            scratch_shapes=[pltpu.VMEM((part_rows, width), jnp.float32), pltpu.VMEM((part_rows, 128), jnp.float32), pltpu.SemaphoreType.DMA((2,))],
        ),
        out_shape=[jax.ShapeDtypeStruct((vocab, width), jnp.float32), jax.ShapeDtypeStruct((vocab, 128), jnp.float32)],
        input_output_aliases=aliases,
        compiler_params=params(),
        cost_estimate=pl.CostEstimate(flops=2 * slots * part_rows * width, bytes_accessed=slots * part_rows * 4, transcendentals=slots * part_rows),
        name="de",
    )(*args)


def combine(stat, weights_row, denom):
    parts = lax.all_gather(stat[:3], "tp", axis=0)
    top = jnp.max(parts[:, 0], axis=0)
    total = jnp.sum(parts[:, 1] * jnp.exp(parts[:, 0] - top[None]), axis=0)
    target = jnp.sum(parts[:, 2], axis=0)
    zero = jnp.zeros_like(top)
    rows = jnp.stack([top, 1.0 / total, weights_row / denom, zero, zero, zero, zero, zero])
    return rows, jnp.log(total) + top - target


def packed(values, index, slots):
    hot = index[..., None, :] == jnp.arange(slots, dtype=jnp.int32)[:, None]
    return jnp.sum(jnp.where(hot, values[..., None, :], 0), axis=-1)


def earlier_of(batch):
    return (jnp.arange(batch)[:, None] > jnp.arange(batch)[None, :]).astype(jnp.float32)


def solution(mesh):
    dp, tp = mesh.shape["dp"], mesh.shape["tp"]

    def share_of(slots, hidden, weights, plan, w_t, b_t, gamma, beta):
        offset, _, _, rowpos_col, seat_row = plan
        share = slots // tp
        low = lax.axis_index("tp") * share
        groups = hidden.shape[0] // GROUP
        first_of = offset.reshape(groups, GROUP)[:, 0]
        ends = first_of + jnp.sum(weights.reshape(groups, -1), axis=1).astype(jnp.int32)
        bounds = jnp.sum(jnp.stack([ends <= low, first_of < low + share]).astype(jnp.int32), axis=1)
        some = pick(hidden, rowpos_col, seat_row, bounds, offset, slots)
        part_rows = lax.dynamic_slice_in_dim(some, low, share, 0)
        pre_act = jnp.dot(part_rows, w_t, preferred_element_type=jnp.float32) + b_t
        return lax.optimization_barrier(gelu_norm(pre_act, gamma, beta).astype(jnp.bfloat16).astype(jnp.float32))

    def body(unrolled, slots, sent, hidden, positions, weights, turned, plan, w_t, b_t, gamma, beta, embed, out_bias):
        batch, seq_len, width = hidden.shape
        max_pred = positions.shape[1]
        shard_vocab = embed.shape[0]
        groups = batch // GROUP
        per_plane = slots // BLOCK_N
        dp_idx, tp_idx = lax.axis_index("dp"), lax.axis_index("tp")
        which = dp_idx.reshape(1).astype(jnp.int32)
        denom = jnp.sum(turned[:, 1]) + LOSS_EPS
        offset, seat, row_of, rowpos_col, seat_row = plan
        before, column = earlier_of(batch), jnp.arange(max_pred, dtype=jnp.int32)

        t_part = share_of(slots, hidden, weights, plan, w_t, b_t, gamma, beta) if sent is None else sent
        t_all = lax.all_gather(t_part, ("dp", "tp"), axis=0, tiled=True)

        turned, held, bias_col, t_part = lax.optimization_barrier((turned, hidden, out_bias, t_part))
        bias_col = bias_col.reshape(-1, 1)
        every = jnp.array([0, groups], jnp.int32)
        tok_rows = pick(held, rowpos_col, seat_row, every, offset, slots)
        pre_act = jnp.dot(tok_rows, w_t, preferred_element_type=jnp.float32) + b_t
        activated, gelu_vjp = jax.vjp(lambda u: jax.nn.gelu(u, approximate=False), pre_act)
        slope = gelu_vjp(jnp.ones_like(pre_act))[0]
        centered = activated - jnp.mean(activated, axis=-1, keepdims=True)
        spread = lax.rsqrt(jnp.mean(centered * centered, axis=-1, keepdims=True) + LN_EPS)
        unit = centered * spread
        t_own = (unit * gamma + beta).astype(jnp.bfloat16)
        slope, unit = lax.optimization_barrier((slope, unit))

        ahead = jnp.sum(jnp.where(before[None] > 0, jnp.sum(turned[:, 1].reshape(dp, 1, batch, max_pred), axis=3), 0.0), axis=2)
        index = jnp.where(turned[:, 1].reshape(dp, batch, max_pred) > 0, ahead[:, :, None].astype(jnp.int32) + column, -1)
        index = index.reshape(dp, batch * max_pred)
        labels = turned[:, 0].astype(jnp.int32) - tp_idx * shard_vocab
        total = jnp.sum(turned[:, 1], axis=1)
        weight_rows = (jnp.arange(slots, dtype=jnp.int32)[None, :] < total[:, None].astype(jnp.int32)).astype(jnp.float32)
        own_lab = packed(labels[:1], index[:1], slots)
        z_own, stat_own = logits_call(unrolled, which, t_own, embed, bias_col, own_lab, 0, per_plane)
        rows_own, ce = combine(stat_own, weight_rows[0], denom)
        dt_part = dt_call(unrolled, z_own, rows_own, own_lab, embed)
        d_normed = lax.psum(dt_part, "tp")
        carry = de_call(unrolled, which, z_own, rows_own, own_lab, t_own, 0, per_plane)
        far_lab = packed(labels[1:], index[1:], slots).reshape(1, -1)
        loss = jnp.sum(weight_rows[0] * ce)

        t_all, carry, far_lab = lax.optimization_barrier((t_all, carry, far_lab))
        z_far, stat_far = logits_call(unrolled, which, t_all, embed, bias_col, far_lab, dp, per_plane)
        rows_far, _ = combine(stat_far, weight_rows[1:].reshape(-1), denom)

        de_sum, db_sum = de_call(unrolled, which, z_far, rows_far, far_lab, t_all, dp, per_plane, carry, 0, 2)

        d_normed, db_sum = lax.optimization_barrier((d_normed, db_sum))
        d_unit = d_normed * gamma
        along = jnp.mean(d_unit * unit, axis=-1, keepdims=True)
        d_act = (d_unit - jnp.mean(d_unit, axis=-1, keepdims=True) - unit * along) * spread
        d_pre = d_act * slope
        d_gamma = jnp.sum(d_normed * unit, axis=0)
        d_beta = jnp.sum(d_normed, axis=0)
        d_pre_bf = d_pre.astype(jnp.bfloat16)
        cut = width // tp
        part_cols = lax.dynamic_slice_in_dim(tok_rows, tp_idx * cut, cut, 1)
        d_w_t = jnp.einsum("nd,ne->de", part_cols, d_pre_bf, preferred_element_type=jnp.float32)
        vecs = [jnp.sum(d_pre, axis=0)[None], d_gamma[None], d_beta[None], jnp.full((5, width), loss)]
        block, d_pre_bf, de_sum, db_sum = lax.optimization_barrier((jnp.concatenate([d_w_t] + vecs), d_pre_bf, de_sum, db_sum))
        block = lax.psum(block, "dp")
        de_sum, db_sum = de_call(unrolled, which, z_far, rows_far, far_lab, t_all, dp, per_plane, (de_sum, db_sum), 1, 2)
        block, d_pre_bf, db_sum = lax.optimization_barrier((block, d_pre_bf, db_sum))
        d_w_t = lax.all_gather(block[:cut], "tp", axis=0, tiled=True)
        d_rows = jnp.einsum("ne,de->nd", d_pre_bf, w_t, preferred_element_type=jnp.float32).astype(jnp.bfloat16)
        d_hidden = put(d_rows, row_of.reshape(groups, 1, -1), seat.reshape(-1, 1), offset, batch, seq_len)
        d_out_bias = jnp.sum(db_sum, axis=1)
        return block[cut + 3, 0] / denom, d_hidden, d_w_t, block[cut], block[cut + 1], block[cut + 2], de_sum, d_out_bias

    def local_step(hidden, positions, labels, weights, w_t, b_t, gamma, beta, embed, out_bias):
        batch, seq_len, _ = hidden.shape
        groups = batch // GROUP
        small = jnp.stack([labels.reshape(-1).astype(jnp.float32), weights.reshape(-1)])
        rings = [[((j + k) % dp, j) for j in range(dp)] for k in range(1, dp)]
        turned = jnp.stack([small] + [lax.ppermute(small, "dp", ring) for ring in rings])

        column = jnp.arange(weights.shape[1], dtype=jnp.int32)
        by_seq = jnp.sum(weights, axis=1)
        offset = jnp.sum(earlier_of(batch) * by_seq[None, :], axis=1).astype(jnp.int32)
        seat = jnp.where(weights > 0, offset[:, None] + column, -WINDOW * batch)
        row_of = positions + (jnp.arange(batch, dtype=jnp.int32) % GROUP * seq_len)[:, None]
        plan = (offset, seat, row_of, row_of.reshape(-1, 1), seat.reshape(groups, 1, -1))
        sent = share_of(PACKED_ROWS, hidden, weights, plan, w_t, b_t, gamma, beta)
        fits = jnp.max(jnp.sum(turned[:, 1], axis=1)) <= PACKED_ROWS
        args = (hidden, positions, weights, turned, plan, w_t, b_t, gamma, beta, embed, out_bias)

        def packed_form(sent, *args):
            return body(True, PACKED_ROWS, sent, *args)

        def whole_form(sent, *args):
            return body(False, labels.size, None, *args)

        return lax.cond(fits, packed_form, whole_form, sent, *args)

    in_specs = (P("dp", None, None), P("dp", None), P("dp", None), P("dp", None), P(None, None), P(None), P(None), P(None), P("tp", None), P("tp"))
    out_specs = (P(), P("dp", None, None), P(None, None), P(None), P(None), P(None), P("tp", None), P("tp"))
    return jax.shard_map(local_step, mesh=mesh, in_specs=in_specs, out_specs=out_specs, check_vma=False)
```
